32 devices in a mesh: seq: 8 (over z, x), head: 4 (over y, core).
Axes of the slice: x: 2, y: 2, z: 4, core: 2. Of those that a mesh axis runs over, the one named last changes fastest.
Arguments:
- query: bfloat16 [4096, 4096], P(('seq', 'head')), may hold values from -6 to 6
- key: bfloat16 [4096, 1024], P(('seq', 'head')), may hold values from -6 to 6
- value: bfloat16 [4096, 1024], P(('seq', 'head')), may hold values from -6 to 6
- out: bfloat16 [4096, 4096], P(('seq', 'head')), may hold values from -4 to 4
- output_gradient: bfloat16 [4096, 4096], P(('seq', 'head')), may hold values from -6 to 6
- log_sum_exp: float32 [4096, 32], P(('seq', 'head')), may hold values from 4 to 7
- segment_ids: int32 [4096], replicated, may hold values from 0 to 3, never falling along the last dimension, each value on 1 to 1536 neighbouring positions
Outputs:
- d_query: bfloat16 [4096, 4096], P(('seq', 'head'))
- key_gradient: bfloat16 [4096, 1024], P(('seq', 'head'))
- value_gradient: bfloat16 [4096, 1024], P(('seq', 'head'))
The draws below stay inside these ranges and needn't reach their ends.
Inputs may be any that keep to these rules, and one draw needn't show every extreme that they name: `segment_ids`: never falls along the positions; a document holds at most 1536 positions, and one holds exactly 1536.
All inputs are finite; a program needn't handle non-finite values.
Results may differ from the reference program's by a relative error of at most 0.0071.
Values may be sent and summed in bfloat16 or wider, within the bound.
A program may use at most 128 MiB of HBM per device.

```python
import math
import jax
import jax.numpy as jnp
import numpy as np
from jax import lax

QUERY_HEADS = 32
KEY_VALUE_HEADS = 8
HEAD_SIZE = 128
TOK_DEV = 128
REACH = 3
PACKED_TOKENS = 4096
MOST = 1536
DOCS = 4
N_HEAD = 4


def block_levels(rng, shape, pieces, low, top_value):
    level, own = 1.0, jax.random.fold_in(rng, 6)
    for axis_at, shards_of in pieces:
        heights = jnp.exp(jax.random.uniform(jax.random.fold_in(own, axis_at), (shards_of,), jnp.float32, low / len(pieces), top_value / len(pieces)))
        level = level * jnp.repeat(heights, shape[axis_at] // shards_of).reshape([-1 if axis == axis_at else 1 for axis in range(len(shape))])
    return level


def split_up(number_of, total, most, slope):
    portions = [(1 << 20) // math.isqrt(rank ** slope) + 1 for rank in range(2, number_of + 1)]
    spare, counts = total - most - (number_of - 1), [1] * (number_of - 1)
    while spare > 0:
        movable = [i for i in range(number_of - 1) if counts[i] < most]
        pool, budget = sum([portions[i] for i in movable]), spare
        for i in movable:
            more = min(most - counts[i], max(1, budget * portions[i] // pool), spare)
            counts[i] = counts[i] + more
            spare = spare - more
    return np.array([most] + counts)


def uneven_parts(key, number_of, total, most, lean):
    if number_of == 2:
        one = jax.random.randint(key, (), max(1, total - most), min(most, total - 1) + 1)
        return jnp.stack([one, total - one])
    sizes = jnp.asarray(split_up(number_of, total, most, lean), jnp.int32)
    couples = (number_of - 1) // 2
    donor, sink = sizes[1:1 + 2 * couples:2], sizes[2:2 + 2 * couples:2]
    slack = jnp.minimum(donor - 1, most - sink)
    moved = jax.random.randint(jax.random.fold_in(key, 1), (couples,), 0, 1 << 20) % (slack + 1)
    sizes = sizes.at[1:1 + 2 * couples:2].set(donor - moved).at[2:2 + 2 * couples:2].set(sink + moved)
    return sizes[jax.random.permutation(jax.random.fold_in(key, 2), number_of)]


def noise(rng, shape, width, bound, cuts=(), kind=jnp.bfloat16):
    level = block_levels(rng, shape, cuts, -0.22, 0.18) if cuts else 1.0
    entries = jax.random.normal(rng, shape, jnp.float32) * width * level
    return jnp.minimum(jnp.maximum(entries, -bound), bound).astype(kind)


def setup_inputs(seed: int = 0) -> dict:
    streams_of = jax.random.split(jax.random.key(seed), 8)
    query = noise(streams_of[0], (PACKED_TOKENS, QUERY_HEADS * HEAD_SIZE), 1.0, 6.0, ((0, 32),))
    key = noise(streams_of[1], (PACKED_TOKENS, KEY_VALUE_HEADS * HEAD_SIZE), 1.0, 6.0, ((0, 32),))
    value = noise(streams_of[2], (PACKED_TOKENS, KEY_VALUE_HEADS * HEAD_SIZE), 1.0, 6.0, ((0, 32),))
    out = noise(streams_of[3], (PACKED_TOKENS, QUERY_HEADS * HEAD_SIZE), 0.5, 4.0, ((0, 32),))
    output_gradient = noise(streams_of[4], (PACKED_TOKENS, QUERY_HEADS * HEAD_SIZE), 1.0, 6.0, ((0, 32),))
    log_sum_exp = jnp.clip(4.0 + 3.0 * jax.random.uniform(streams_of[5], (PACKED_TOKENS, QUERY_HEADS), jnp.float32) ** block_levels(streams_of[5], (PACKED_TOKENS, QUERY_HEADS), ((0, 32),), -0.2, 0.2), 4.0, 7.0)
    segment_ids = jnp.searchsorted(jnp.cumsum(uneven_parts(streams_of[6], DOCS, PACKED_TOKENS, MOST, 2)), jnp.arange(PACKED_TOKENS), side="right").astype(jnp.int32)
    return {"query": query, "key": key, "value": value, "out": out, "output_gradient": output_gradient, "log_sum_exp": log_sum_exp, "segment_ids": segment_ids}


def rounded(values):
    return lax.optimization_barrier(values.astype(jnp.bfloat16)).astype(jnp.float32)

def reference(query, key, value, out, output_gradient, log_sum_exp, segment_ids):
    row_number = TOK_DEV * N_HEAD
    block_list = PACKED_TOKENS // row_number
    group_width = QUERY_HEADS // KEY_VALUE_HEADS
    score_scale = 1.0 / math.sqrt(HEAD_SIZE)
    padding_rows = REACH * row_number
    window_rows = (REACH + 1) * row_number
    query_total = query.astype(jnp.float32).reshape(block_list, row_number, KEY_VALUE_HEADS, group_width, HEAD_SIZE)
    gradient_total = output_gradient.astype(jnp.float32).reshape(block_list, row_number, KEY_VALUE_HEADS, group_width, HEAD_SIZE)
    output_total = out.astype(jnp.float32).reshape(block_list, row_number, KEY_VALUE_HEADS, group_width, HEAD_SIZE)
    delta_all = lax.optimization_barrier(jnp.sum(gradient_total * output_total, axis=4))
    log_sum_exp_total = log_sum_exp.astype(jnp.float32).reshape(block_list, row_number, KEY_VALUE_HEADS, group_width)
    key_padded = jnp.concatenate([jnp.zeros((padding_rows, KEY_VALUE_HEADS * HEAD_SIZE), jnp.float32), key.astype(jnp.float32)], axis=0).reshape(padding_rows + PACKED_TOKENS, KEY_VALUE_HEADS, HEAD_SIZE)
    value_padded = jnp.concatenate([jnp.zeros((padding_rows, KEY_VALUE_HEADS * HEAD_SIZE), jnp.float32), value.astype(jnp.float32)], axis=0).reshape(padding_rows + PACKED_TOKENS, KEY_VALUE_HEADS, HEAD_SIZE)
    seg_ids = segment_ids.astype(jnp.int32)
    seg_pad = jnp.concatenate([jnp.full((padding_rows,), -1, jnp.int32), seg_ids])
    query_offsets = jnp.arange(row_number, dtype=jnp.int32) + padding_rows
    key_offsets = jnp.arange(window_rows, dtype=jnp.int32)

    def block_step(accums, inputs):
        key_gradient_total, value_gradient_total = accums
        query_heads, grad_heads, delta_rows, lse_rows, index = inputs
        window_start = (index * row_number).astype(jnp.int32)
        key_block = lax.dynamic_slice_in_dim(key_padded, window_start, window_rows, 0)
        value_block = lax.dynamic_slice_in_dim(value_padded, window_start, window_rows, 0)
        seg_keys = lax.dynamic_slice_in_dim(seg_pad, window_start, window_rows, 0)
        seg_query = lax.dynamic_slice_in_dim(seg_ids, window_start, row_number, 0)
        allowed = (seg_query[:, None] == seg_keys[None, :]) & (key_offsets[None, :] <= query_offsets[:, None])
        lse_cols = lse_rows.transpose(1, 2, 0)[..., None]
        delta_cols = delta_rows.transpose(1, 2, 0)[..., None]
        scores = jnp.einsum('igmd,jgd->gmij', query_heads, key_block) * score_scale
        probs = jnp.exp(jnp.where(allowed, scores - lse_cols, -jnp.inf))
        probs_low = rounded(probs)
        dprobs = jnp.einsum('igmd,jgd->gmij', grad_heads, value_block)
        dscores = rounded(score_scale * probs * (dprobs - delta_cols))
        grad_query = jnp.einsum('gmij,jgd->igmd', dscores, key_block)
        grad_key = jnp.einsum('gmij,igmd->jgd', dscores, query_heads)
        grad_value = jnp.einsum('gmij,igmd->jgd', probs_low, grad_heads)
        key_gradient_total = lax.dynamic_update_slice_in_dim(key_gradient_total, lax.dynamic_slice_in_dim(key_gradient_total, window_start, window_rows, 0) + grad_key, window_start, 0)
        value_gradient_total = lax.dynamic_update_slice_in_dim(value_gradient_total, lax.dynamic_slice_in_dim(value_gradient_total, window_start, window_rows, 0) + grad_value, window_start, 0)
        return ((key_gradient_total, value_gradient_total), grad_query.astype(jnp.bfloat16))
    starting_totals = (jnp.zeros((padding_rows + PACKED_TOKENS, KEY_VALUE_HEADS, HEAD_SIZE), jnp.float32), jnp.zeros((padding_rows + PACKED_TOKENS, KEY_VALUE_HEADS, HEAD_SIZE), jnp.float32))
    indices = jnp.arange(block_list, dtype=jnp.int32)
    (key_gradient_total, value_gradient_total), grad_blocks = lax.scan(block_step, starting_totals, (query_total, gradient_total, delta_all, log_sum_exp_total, indices))
    d_query = grad_blocks.reshape(PACKED_TOKENS, QUERY_HEADS * HEAD_SIZE)
    key_gradient = key_gradient_total[padding_rows:].reshape(PACKED_TOKENS, KEY_VALUE_HEADS * HEAD_SIZE).astype(jnp.bfloat16)
    value_gradient = value_gradient_total[padding_rows:].reshape(PACKED_TOKENS, KEY_VALUE_HEADS * HEAD_SIZE).astype(jnp.bfloat16)
    return (d_query, key_gradient, value_gradient)
```

```python
import functools
import math

import jax
import jax.numpy as jnp
from jax import lax
from jax.experimental import pallas as pl
from jax.experimental.pallas import tpu as pltpu
from jax.sharding import PartitionSpec as P

HEAD_SIZE = 128
REACH = 3
TILE = 256
LOG2E = math.log2(math.e)
MESH = pl.DeviceIdType.MESH
NT = (((1,), (1,)), ((), ()))


def dot(a, b):
    return jnp.dot(a, b, preferred_element_type=jnp.float32)


def dot_nt(a, b):
    return lax.dot_general(a, b, NT, preferred_element_type=jnp.float32)


def kernel(
    n, seqs, groups, width,
    q_ref, e_ref, k_ref, v_ref, st_ref, start_ref,
    dq_out, dk_out, dv_out,
    qb, eb, stb, kw, vw, dqt, acck, accv, ownk, ownv, part_s, part_r, dqs, dks, dvs,
    loc_sem, in_s, in_r, fw_s, fw_r, pt_s, pt_r, out_s, out_r,
):
    s = lax.axis_index("seq")
    h = lax.axis_index("head")
    rows = q_ref.shape[0]
    block = rows * n
    cols = q_ref.shape[1] // n
    kcols = k_ref.shape[1] // n
    hd = HEAD_SIZE
    gw = width * hd
    halves = block // TILE
    scale = 1.0 / math.sqrt(hd)
    heads = groups * width

    def at(index, size):
        return pl.ds(pl.multiple_of(index * size, size), size)

    barrier = pltpu.get_barrier_semaphore()
    for r in range(1, n):
        pl.semaphore_signal(barrier, inc=1, device_id={"head": lax.rem(h + r, n)}, device_id_type=MESH)
    for d in range(1, REACH + 1):
        @pl.when(s + d < seqs)
        def _():
            pl.semaphore_signal(barrier, inc=1, device_id={"seq": s + d}, device_id_type=MESH)

        @pl.when(s >= d)
        def _():
            pl.semaphore_signal(barrier, inc=1, device_id={"seq": s - d}, device_id_type=MESH)
    pl.semaphore_wait(barrier, n - 1 + jnp.minimum(s, REACH) + jnp.minimum(seqs - 1 - s, REACH))

    def entry(kind, owner, me):
        if kind == 0:
            return st_ref.at[owner], stb.at[:, at(me, rows)]
        if kind == 1:
            return k_ref.at[:, at(owner, kcols)], kw.at[0, at(me, rows), :]
        if kind == 2:
            return v_ref.at[:, at(owner, kcols)], vw.at[0, at(me, rows), :]
        g, which = (kind - 3) // 2, (kind - 3) % 2
        src, dst = ((q_ref, qb), (e_ref, eb))[which]
        from_cols = pl.ds(pl.multiple_of(owner * cols + g * gw, hd), gw)
        return src.at[:, from_cols], dst.at[at(me, rows), pl.ds(g * gw, gw)]

    kinds = 3 + 2 * groups

    def entry_copy(kind, r):
        peer = lax.rem(h + r, n)
        src, dst = entry(kind, peer, h)
        return pltpu.make_async_remote_copy(
            src_ref=src, dst_ref=dst, send_sem=in_s.at[kind, r - 1], recv_sem=in_r.at[kind, r - 1],
            device_id={"head": peer}, device_id_type=MESH)

    def entry_own(kind):
        src, dst = entry(kind, h, h)
        return pltpu.make_async_copy(src, dst, loc_sem.at[kind])

    for kind in (1, 2, 0) + tuple(range(3, kinds)):
        entry_own(kind).start()
        for r in range(1, n):
            entry_copy(kind, r).start()

    def entry_wait(kind):
        entry_own(kind).wait()
        for r in range(1, n):
            entry_copy(kind, r).wait_recv()

    def forward(which, d):
        buf = (kw, vw)[which]
        return pltpu.make_async_remote_copy(
            src_ref=buf.at[0], dst_ref=buf.at[d], send_sem=fw_s.at[which, d - 1], recv_sem=fw_r.at[which, d - 1],
            device_id={"seq": s + d}, device_id_type=MESH)

    def partial(which, g, d):
        return pltpu.make_async_remote_copy(
            src_ref=part_s.at[which, g, d - 1], dst_ref=part_r.at[which, g, d - 1],
            send_sem=pt_s.at[which, g, d - 1], recv_sem=pt_r.at[which, g, d - 1],
            device_id={"seq": s - d}, device_id_type=MESH)

    def leave(which, g, owner):
        src, dst, size, full = ((dqs, dq_out, gw, cols), (dks, dk_out, hd, kcols), (dvs, dv_out, hd, kcols))[which]
        to_cols = pl.ds(pl.multiple_of(h * full + g * size, hd), size)
        return src.at[at(owner, rows), pl.ds(g * size, size)], dst.at[:, to_cols]

    def leave_copy(which, g, r):
        peer = lax.rem(h + r, n)
        src, dst = leave(which, g, peer)
        return pltpu.make_async_remote_copy(
            src_ref=src, dst_ref=dst, send_sem=out_s.at[which, g, r - 1], recv_sem=out_r.at[which, g, r - 1],
            device_id={"head": peer}, device_id_type=MESH)

    def leave_own(which, g):
        src, dst = leave(which, g, h)
        return pltpu.make_async_copy(src, dst, loc_sem.at[kinds + which * groups + g])

    def leave_start(which, g):
        for r in range(1, n):
            leave_copy(which, g, r).start()
        leave_own(which, g).start()

    for kind in (1, 2):
        entry_wait(kind)
    for d in range(1, REACH + 1):
        @pl.when(s + d < seqs)
        def _():
            forward(0, d).start()
            forward(1, d).start()
    entry_wait(0)

    row_at = lax.broadcasted_iota(jnp.int32, (TILE, TILE), 0)
    col_at = lax.broadcasted_iota(jnp.int32, (TILE, TILE), 1)

    def tile(g, d, hf, qt):
        k_rows, q_rows = at(hf, TILE), at(qt, TILE)
        kcol = pl.ds(g * hd, hd)
        key, val = kw[d, k_rows, kcol], vw[d, k_rows, kcol]
        key_t = key.T
        first = start_ref[0:1, q_rows] - (hf * TILE - d * block)
        allowed = row_at >= first
        if d == 0:
            allowed &= row_at + (hf - qt) * TILE <= col_at
        add_k = add_v = None
        for m in range(width):
            hcol = pl.ds((g * width + m) * hd, hd)
            query, grad = qb[q_rows, hcol], eb[q_rows, hcol]
            lse = stb[g * width + m : g * width + m + 1, q_rows]
            delta = stb[heads + g * width + m : heads + g * width + m + 1, q_rows]
            scores = dot_nt(key, query)
            probs = jnp.exp2(jnp.where(allowed, scores * (scale * LOG2E) - lse, -jnp.inf))
            dprobs = dot_nt(val, grad)
            dscores = (probs * (dprobs - delta)).astype(jnp.bfloat16)
            one_v = dot(probs.astype(jnp.bfloat16), grad)
            one_k = dot(dscores, query)
            add_v = one_v if m == 0 else add_v + one_v
            add_k = one_k if m == 0 else add_k + one_k
            dqt[m, :, q_rows] += dot(key_t, dscores)
        acck[k_rows, :] += add_k
        accv[k_rows, :] += add_v

    def compute(g, d):
        acck[...] = jnp.zeros_like(acck)
        accv[...] = jnp.zeros_like(accv)

        @pl.loop(0, halves)
        def _(hf):
            low = hf if d == 0 else 0
            high = hf + 1 if d == REACH else halves

            @pl.loop(low, high)
            def _(qt):
                tile(g, d, hf, qt)

    def finish(g):
        for d in range(1, REACH + 1):
            @pl.when(s + d < seqs)
            def _():
                partial(0, g, d).wait_recv()
                partial(1, g, d).wait_recv()
                ownk[g] += part_r[0, g, d - 1].astype(jnp.float32)
                ownv[g] += part_r[1, g, d - 1].astype(jnp.float32)
        dks[:, g * hd : (g + 1) * hd] = (ownk[g] * scale).astype(jnp.bfloat16)
        dvs[:, g * hd : (g + 1) * hd] = ownv[g].astype(jnp.bfloat16)
        leave_start(1, g)
        leave_start(2, g)

    for g in range(groups):
        entry_wait(3 + 2 * g)
        entry_wait(4 + 2 * g)
        dqt[...] = jnp.zeros_like(dqt)
        order = range(REACH + 1) if g == 0 else range(REACH, -1, -1)
        for step, d in enumerate(order):
            if d == 0:
                compute(g, 0)
                ownk[g] = acck[...]
                ownv[g] = accv[...]
            else:
                @pl.when(s >= d)
                def _():
                    if g == 0:
                        forward(0, d).wait_recv()
                        forward(1, d).wait_recv()
                    compute(g, d)
                    part_s[0, g, d - 1] = acck[...].astype(jnp.bfloat16)
                    part_s[1, g, d - 1] = accv[...].astype(jnp.bfloat16)
                    partial(0, g, d).start()
                    partial(1, g, d).start()
            if g > 0 and step == 1:
                finish(g - 1)
        for m in range(width):
            here = (g * width + m) * hd
            dqs[:, here : here + hd] = (dqt[m] * scale).T.astype(jnp.bfloat16)
        leave_start(0, g)
    finish(groups - 1)

    for which in range(3):
        for g in range(groups):
            leave_own(which, g).wait()
            for r in range(1, n):
                leave_copy(which, g, r).wait()
    for kind in range(kinds):
        for r in range(1, n):
            entry_copy(kind, r).wait_send()
    for d in range(1, REACH + 1):
        @pl.when(s + d < seqs)
        def _():
            forward(0, d).wait_send()
            forward(1, d).wait_send()

        @pl.when(s >= d)
        def _():
            for g in range(groups):
                partial(0, g, d).wait_send()
                partial(1, g, d).wait_send()


def shards(query, key, value, out, output_gradient, log_sum_exp, segment_ids):
    n, seqs = lax.axis_size("head"), lax.axis_size("seq")
    hd = HEAD_SIZE
    rows = query.shape[0]
    block = rows * n
    cols, kcols = query.shape[1] // n, key.shape[1] // n
    groups, width = kcols // hd, cols // kcols
    heads = groups * width
    delta = jnp.sum(
        (output_gradient.astype(jnp.float32) * out.astype(jnp.float32)).reshape(rows, -1, hd), axis=2
    )
    stats = jnp.concatenate(
        [(log_sum_exp * LOG2E).T.reshape(n, heads, rows), delta.T.reshape(n, heads, rows)], axis=1
    )
    base = lax.axis_index("seq") * block
    mine = lax.dynamic_slice_in_dim(segment_ids, base, block, 0)
    start = jnp.sum((segment_ids[:, None] < mine[None, :]).astype(jnp.int32), axis=0)[None, :] - base
    bf16, f32 = jnp.bfloat16, jnp.float32
    kinds = 3 + 2 * groups
    vmem = pl.BlockSpec(memory_space=pltpu.VMEM)
    dma = pltpu.SemaphoreType.DMA
    return pl.pallas_call(
        functools.partial(kernel, n, seqs, groups, width),
        out_shape=[
            jax.ShapeDtypeStruct(query.shape, bf16),
            jax.ShapeDtypeStruct(key.shape, bf16),
            jax.ShapeDtypeStruct(value.shape, bf16),
        ],
        in_specs=[vmem] * 6,
        out_specs=[vmem] * 3,
        scratch_shapes=[
            pltpu.VMEM((block, cols), bf16),
            pltpu.VMEM((block, cols), bf16),
            pltpu.VMEM((2 * heads, block), f32),
            pltpu.VMEM((REACH + 1, block, kcols), bf16),
            pltpu.VMEM((REACH + 1, block, kcols), bf16),
            pltpu.VMEM((width, hd, block), f32),
            pltpu.VMEM((block, hd), f32),
            pltpu.VMEM((block, hd), f32),
            pltpu.VMEM((groups, block, hd), f32),
            pltpu.VMEM((groups, block, hd), f32),
            pltpu.VMEM((2, groups, REACH, block, hd), bf16),
            pltpu.VMEM((2, groups, REACH, block, hd), bf16),
            pltpu.VMEM((block, cols), bf16),
            pltpu.VMEM((block, kcols), bf16),
            pltpu.VMEM((block, kcols), bf16),
            dma((kinds + 3 * groups,)),
            dma((kinds, n - 1)),
            dma((kinds, n - 1)),
            dma((2, REACH)),
            dma((2, REACH)),
            dma((2, groups, REACH)),
            dma((2, groups, REACH)),
            dma((3, groups, n - 1)),
            dma((3, groups, n - 1)),
        ],
        compiler_params=pltpu.CompilerParams(collective_id=0, has_side_effects=True),
    )(query, output_gradient, key, value, stats, start)


def solution(mesh):
    placed = (P(("seq", "head"), None),) * 6 + (P(),)
    return jax.shard_map(
        lambda *a: tuple(shards(*a)),
        mesh=mesh,
        in_specs=placed,
        out_specs=(P(("seq", "head"), None),) * 3,
        check_vma=False,
    )
```

```python
import functools
import math

import jax
import jax.numpy as jnp
from jax import lax
from jax.experimental import pallas as pl
from jax.experimental.pallas import tpu as pltpu
from jax.sharding import PartitionSpec as P

HEAD_SIZE = 128
REACH = 3
TILE = 256
LOG2E = math.log2(math.e)
MESH = pl.DeviceIdType.MESH
NT = (((1,), (1,)), ((), ()))


def dot(a, b):
    return jnp.dot(a, b, preferred_element_type=jnp.float32)


def dot_nt(a, b):
    return lax.dot_general(a, b, NT, preferred_element_type=jnp.float32)


def kernel(
    n, seqs, groups, width,
    q_ref, e_ref, k_ref, v_ref, st_ref, start_ref,
    dq_out, dk_out, dv_out,
    qb, eb, stb, kv, dqt, acck, accv, ownk, ownv, part_s, part_r, dqs, dks, dvs,
    loc_sem, in_s, in_r, fw_s, fw_r, pt_s, pt_r, out_s, out_r,
):
    s = lax.axis_index("seq")
    h = lax.axis_index("head")
    rows = q_ref.shape[0]
    block = rows * n
    cols = q_ref.shape[1] // n
    kcols = k_ref.shape[1] // n
    hd = HEAD_SIZE
    gw = width * hd
    halves = block // TILE
    scale = 1.0 / math.sqrt(hd)
    heads = groups * width

    def at(index, size):
        return pl.ds(index * size if isinstance(index, int) else pl.multiple_of(index * size, size), size)

    side = s + 1 - 2 * lax.rem(s, 2)
    even = lax.rem(s, 2) == 0
    odd = lax.rem(s, 2) == 1
    has_up, has_down = s + 2 < seqs, s >= 2

    barrier = pltpu.get_barrier_semaphore()
    for r in range(1, n):
        pl.semaphore_signal(barrier, inc=1, device_id={"head": lax.rem(h + r, n)}, device_id_type=MESH)
    pl.semaphore_signal(barrier, inc=1, device_id={"seq": side}, device_id_type=MESH)

    @pl.when(has_up)
    def _():
        pl.semaphore_signal(barrier, inc=1, device_id={"seq": s + 2}, device_id_type=MESH)

    @pl.when(has_down)
    def _():
        pl.semaphore_signal(barrier, inc=1, device_id={"seq": s - 2}, device_id_type=MESH)

    pl.semaphore_wait(barrier, n + jnp.minimum(s // 2, 1) + jnp.minimum((seqs - 1 - s) // 2, 1))

    def entry(kind, owner, me):
        if kind == 0:
            return st_ref.at[owner], stb.at[:, at(me, rows)]
        if kind < first_wide:
            g, which = (kind - 1) // 2, (kind - 1) % 2
            from_cols = pl.ds(pl.multiple_of(owner * kcols + g * hd, hd), hd)
            return (k_ref, v_ref)[which].at[:, from_cols], kv.at[0, g, which, at(me, rows), :]
        g, which = (kind - first_wide) // 2, (kind - first_wide) % 2
        src, dst = ((q_ref, qb), (e_ref, eb))[which]
        from_cols = pl.ds(pl.multiple_of(owner * cols + g * gw, hd), gw)
        return src.at[:, from_cols], dst.at[at(me, rows), pl.ds(g * gw, gw)]

    first_wide = 1 + 2 * groups
    kinds = 1 + 4 * groups

    def entry_copy(kind, r):
        peer = lax.rem(h + r, n)
        src, dst = entry(kind, peer, h)
        return pltpu.make_async_remote_copy(
            src_ref=src, dst_ref=dst, send_sem=in_s.at[kind, r - 1], recv_sem=in_r.at[kind, r - 1],
            device_id={"head": peer}, device_id_type=MESH)

    def entry_own(kind):
        src, dst = entry(kind, h, h)
        return pltpu.make_async_copy(src, dst, loc_sem.at[kind])

    for kind in tuple(range(1, first_wide)) + (0,) + tuple(range(first_wide, kinds)):
        entry_own(kind).start()
        for r in range(1, n):
            entry_copy(kind, r).start()

    def entry_wait(kind):
        entry_own(kind).wait()
        for r in range(1, n):
            entry_copy(kind, r).wait_recv()

    def hand(g, step, slot, to_slot, to):
        return pltpu.make_async_remote_copy(
            src_ref=kv.at[slot, g], dst_ref=kv.at[to_slot, g], send_sem=fw_s.at[g, step],
            recv_sem=fw_r.at[g, to_slot - 1], device_id={"seq": to}, device_id_type=MESH)

    def hand_steps(g):
        return (
            (has_up, hand(g, 0, 0, 2, s + 2)),
            (even, hand(g, 1, 0, 1, side)),
            (has_down & odd, hand(g, 2, 2, 1, side)),
            (has_down & even, hand(g, 2, 2, 3, side)),
            (has_down & even & has_up, hand(g, 3, 1, 3, s + 2)),
        )

    def hand_start(g, steps):
        for i in steps:
            cond, copy = hand_steps(g)[i]

            @pl.when(cond)
            def _():
                copy.start()

    def got(g, d):
        @pl.when(s >= d)
        def _():
            hand(g, 0, 0, d, side).wait_recv()

    def back(g, d, into, to):
        return pltpu.make_async_remote_copy(
            src_ref=part_s.at[g, d - 1], dst_ref=part_r.at[g, into], send_sem=pt_s.at[g, d - 1],
            recv_sem=pt_r.at[g, into], device_id={"seq": to}, device_id_type=MESH)

    def join(g, into):
        back(g, 1, into, side).wait_recv()
        acck[...] += part_r[g, into, 0].astype(jnp.float32)
        accv[...] += part_r[g, into, 1].astype(jnp.float32)

    def put(g, d):
        part_s[g, d - 1, 0] = acck[...].astype(jnp.bfloat16)
        part_s[g, d - 1, 1] = accv[...].astype(jnp.bfloat16)

    def pass_back(g, d):
        if d == 3:
            put(g, 3)

            @pl.when(even)
            def _():
                back(g, 3, 0, s - 2).start()

            @pl.when(odd)
            def _():
                back(g, 3, 1, side).start()
        elif d == 1:
            @pl.when(has_down & even & has_up)
            def _():
                join(g, 0)

            put(g, 1)

            @pl.when(even)
            def _():
                back(g, 1, 1, side).start()

            @pl.when(odd)
            def _():
                back(g, 1, 3, side).start()
        else:
            join(g, 1)
            put(g, 2)
            back(g, 2, 2, s - 2).start()

    def leave(which, g, owner):
        src, dst, size, full = ((dqs, dq_out, gw, cols), (dks, dk_out, hd, kcols), (dvs, dv_out, hd, kcols))[which]
        to_cols = pl.ds(pl.multiple_of(h * full + g * size, hd), size)
        return src.at[at(owner, rows), pl.ds(g * size, size)], dst.at[:, to_cols]

    def leave_copy(which, g, r):
        peer = lax.rem(h + r, n)
        src, dst = leave(which, g, peer)
        return pltpu.make_async_remote_copy(
            src_ref=src, dst_ref=dst, send_sem=out_s.at[which, g, r - 1], recv_sem=out_r.at[which, g, r - 1],
            device_id={"head": peer}, device_id_type=MESH)

    def leave_own(which, g):
        src, dst = leave(which, g, h)
        return pltpu.make_async_copy(src, dst, loc_sem.at[kinds + which * groups + g])

    def leave_start(which, g):
        for r in range(1, n):
            leave_copy(which, g, r).start()
        leave_own(which, g).start()

    for g in range(groups):
        entry_wait(1 + 2 * g)
        entry_wait(2 + 2 * g)
        hand_start(g, (0, 1))
    entry_wait(0)

    def relay_two(g):
        got(g, 2)
        hand_start(g, (2, 3))

    def relay_one(g):
        got(g, 1)
        hand_start(g, (4,))

    row_at = lax.broadcasted_iota(jnp.int32, (TILE, TILE), 0)
    col_at = lax.broadcasted_iota(jnp.int32, (TILE, TILE), 1)

    def tile(g, d, hf, qt):
        k_rows, q_rows = at(hf, TILE), at(qt, TILE)
        key, val = kv[d, g, 0, k_rows, :], kv[d, g, 1, k_rows, :]
        key_t = key.T
        first = start_ref[0:1, q_rows] - (hf * TILE - d * block)
        allowed = row_at >= first
        if d == 0:
            allowed &= row_at + (hf - qt) * TILE <= col_at
        add_k = add_v = None
        for m in range(width):
            hcol = pl.ds((g * width + m) * hd, hd)
            query, grad = qb[q_rows, hcol], eb[q_rows, hcol]
            lse = stb[g * width + m : g * width + m + 1, q_rows]
            delta = stb[heads + g * width + m : heads + g * width + m + 1, q_rows]
            scores = dot_nt(key, query)
            probs = jnp.exp2(jnp.where(allowed, scores * (scale * LOG2E) - lse, -jnp.inf))
            dprobs = dot_nt(val, grad)
            dscores = (probs * (dprobs - delta)).astype(jnp.bfloat16)
            one_v = dot(probs.astype(jnp.bfloat16), grad)
            one_k = dot(dscores, query)
            add_v = one_v if m == 0 else add_v + one_v
            add_k = one_k if m == 0 else add_k + one_k
            dqt[m, :, q_rows] += dot(key_t, dscores)
        acck[k_rows, :] += add_k
        accv[k_rows, :] += add_v

    def compute(g, d):
        acck[...] = jnp.zeros_like(acck)
        accv[...] = jnp.zeros_like(accv)

        for hf in range(halves):
            low = hf if d == 0 else 0
            high = hf + 1 if d == REACH else halves
            for qt in range(low, high):
                tile(g, d, hf, qt)

    def finish(g):
        for cond, into in ((even, 3), (has_up, 2)):
            @pl.when(cond)
            def _():
                back(g, 1, into, side).wait_recv()
                ownk[g] += part_r[g, into, 0].astype(jnp.float32)
                ownv[g] += part_r[g, into, 1].astype(jnp.float32)

        dks[:, g * hd : (g + 1) * hd] = (ownk[g] * scale).astype(jnp.bfloat16)
        dvs[:, g * hd : (g + 1) * hd] = ownv[g].astype(jnp.bfloat16)
        leave_start(1, g)
        leave_start(2, g)

    relay_two(0)
    for g in range(groups):
        if g == 0:
            relay_two(1)
            relay_one(0)
        entry_wait(first_wide + 2 * g)
        entry_wait(first_wide + 1 + 2 * g)
        dqt[...] = jnp.zeros_like(dqt)
        for step, d in enumerate((0, 3, 1, 2) if g == 0 else (3, 1, 2, 0)):
            if d == 0:
                compute(g, 0)
                ownk[g] = acck[...]
                ownv[g] = accv[...]
                if g == 0:
                    relay_one(1)
            else:
                if d == 3:
                    got(g, 3)

                @pl.when(s >= d)
                def _():
                    compute(g, d)
                    pass_back(g, d)
            if g > 0 and step == 1:
                finish(g - 1)
        for m in range(width):
            here = (g * width + m) * hd
            dqs[:, here : here + hd] = (dqt[m] * scale).T.astype(jnp.bfloat16)
        leave_start(0, g)
    finish(groups - 1)

    for which in range(3):
        for g in range(groups):
            leave_own(which, g).wait()
            for r in range(1, n):
                leave_copy(which, g, r).wait()
    for kind in range(kinds):
        for r in range(1, n):
            entry_copy(kind, r).wait_send()
    for g in range(groups):
        for cond, copy in hand_steps(g):
            @pl.when(cond)
            def _():
                copy.wait_send()

        for d in range(1, REACH + 1):
            @pl.when(s >= d)
            def _():
                back(g, d, 0, side).wait_send()


def shards(query, key, value, out, output_gradient, log_sum_exp, segment_ids):
    n, seqs = lax.axis_size("head"), lax.axis_size("seq")
    hd = HEAD_SIZE
    rows = query.shape[0]
    block = rows * n
    cols, kcols = query.shape[1] // n, key.shape[1] // n
    groups, width = kcols // hd, cols // kcols
    heads = groups * width
    delta = jnp.sum(
        (output_gradient.astype(jnp.float32) * out.astype(jnp.float32)).reshape(rows, -1, hd), axis=2
    )
    stats = jnp.concatenate(
        [(log_sum_exp * LOG2E).T.reshape(n, heads, rows), delta.T.reshape(n, heads, rows)], axis=1
    )
    base = lax.axis_index("seq") * block
    mine = lax.dynamic_slice_in_dim(segment_ids, base, block, 0)
    start = jnp.sum((segment_ids[:, None] < mine[None, :]).astype(jnp.int32), axis=0)[None, :] - base
    bf16, f32 = jnp.bfloat16, jnp.float32
    kinds = 1 + 4 * groups
    vmem = pl.BlockSpec(memory_space=pltpu.VMEM)
    dma = pltpu.SemaphoreType.DMA
    return pl.pallas_call(
        functools.partial(kernel, n, seqs, groups, width),
        out_shape=[
            jax.ShapeDtypeStruct(query.shape, bf16),
            jax.ShapeDtypeStruct(key.shape, bf16),
            jax.ShapeDtypeStruct(value.shape, bf16),
        ],
        in_specs=[vmem] * 6,
        out_specs=[vmem] * 3,
        scratch_shapes=[
            pltpu.VMEM((block, cols), bf16),
            pltpu.VMEM((block, cols), bf16),
            pltpu.VMEM((2 * heads, block), f32),
            pltpu.VMEM((REACH + 1, groups, 2, block, hd), bf16),
            pltpu.VMEM((width, hd, block), f32),
            pltpu.VMEM((block, hd), f32),
            pltpu.VMEM((block, hd), f32),
            pltpu.VMEM((groups, block, hd), f32),
            pltpu.VMEM((groups, block, hd), f32),
            pltpu.VMEM((groups, REACH, 2, block, hd), bf16),
            pltpu.VMEM((groups, REACH + 1, 2, block, hd), bf16),
            pltpu.VMEM((block, cols), bf16),
            pltpu.VMEM((block, kcols), bf16),
            pltpu.VMEM((block, kcols), bf16),
            dma((kinds + 3 * groups,)),
            dma((kinds, n - 1)),
            dma((kinds, n - 1)),
            dma((groups, REACH + 1)),
            dma((groups, REACH)),
            dma((groups, REACH)),
            dma((groups, REACH + 1)),
            dma((3, groups, n - 1)),
            dma((3, groups, n - 1)),
        ],
        compiler_params=pltpu.CompilerParams(collective_id=0, has_side_effects=True),
    )(query, output_gradient, key, value, stats, start)


def solution(mesh):
    placed = (P(("seq", "head"), None),) * 6 + (P(),)
    return jax.shard_map(
        lambda *a: tuple(shards(*a)),
        mesh=mesh,
        in_specs=placed,
        out_specs=(P(("seq", "head"), None),) * 3,
        check_vma=False,
    )
```

```python
import functools
import math

import jax
import jax.numpy as jnp
from jax import lax
from jax.experimental import pallas as pl
from jax.experimental.pallas import tpu as pltpu
from jax.sharding import PartitionSpec as P

HEAD_SIZE = 128
REACH = 3
TILE = 256
LOG2E = math.log2(math.e)
MESH = pl.DeviceIdType.MESH
NT = (((1,), (1,)), ((), ()))


def dot(a, b):
    return jnp.dot(a, b, preferred_element_type=jnp.float32)


def dot_nt(a, b):
    return lax.dot_general(a, b, NT, preferred_element_type=jnp.float32)


def kernel(
    n, seqs, groups, width,
    q_ref, e_ref, k_ref, v_ref, o_ref, lse_ref, start_ref,
    dq_out, dk_out, dv_out,
    st_ref, qb, eb, stb, kv, dqt, acck, accv, ownk, ownv, part_s, part_r, dqs, dks, dvs,
    loc_sem, in_s, in_r, fw_s, fw_r, pt_s, pt_r, out_s, out_r,
):
    s = lax.axis_index("seq")
    h = lax.axis_index("head")
    rows = q_ref.shape[0]
    block = rows * n
    cols = q_ref.shape[1] // n
    kcols = k_ref.shape[1] // n
    hd = HEAD_SIZE
    gw = width * hd
    halves = block // TILE
    scale = 1.0 / math.sqrt(hd)
    heads = groups * width

    def at(index, size):
        return pl.ds(index * size if isinstance(index, int) else pl.multiple_of(index * size, size), size)

    side = s + 1 - 2 * lax.rem(s, 2)
    even = lax.rem(s, 2) == 0
    odd = lax.rem(s, 2) == 1
    has_up, has_down = s + 2 < seqs, s >= 2

    barrier = pltpu.get_barrier_semaphore()
    for r in range(1, n):
        pl.semaphore_signal(barrier, inc=1, device_id={"head": lax.rem(h + r, n)}, device_id_type=MESH)
    pl.semaphore_signal(barrier, inc=1, device_id={"seq": side}, device_id_type=MESH)

    @pl.when(has_up)
    def _():
        pl.semaphore_signal(barrier, inc=1, device_id={"seq": s + 2}, device_id_type=MESH)

    @pl.when(has_down)
    def _():
        pl.semaphore_signal(barrier, inc=1, device_id={"seq": s - 2}, device_id_type=MESH)

    pl.semaphore_wait(barrier, n + jnp.minimum(s // 2, 1) + jnp.minimum((seqs - 1 - s) // 2, 1))

    def entry(kind, owner, me):
        if kind == 0:
            return st_ref.at[owner], stb.at[:, at(me, rows)]
        if kind < first_wide:
            g, which = (kind - 1) // 2, (kind - 1) % 2
            from_cols = pl.ds(pl.multiple_of(owner * kcols + g * hd, hd), hd)
            return (k_ref, v_ref)[which].at[:, from_cols], kv.at[0, g, which, at(me, rows), :]
        g, which = (kind - first_wide) // 2, (kind - first_wide) % 2
        src, dst = ((q_ref, qb), (e_ref, eb))[which]
        from_cols = pl.ds(pl.multiple_of(owner * cols + g * gw, hd), gw)
        return src.at[:, from_cols], dst.at[at(me, rows), pl.ds(g * gw, gw)]

    first_wide = 1 + 2 * groups
    kinds = 1 + 4 * groups

    def entry_copy(kind, r):
        peer = lax.rem(h + r, n)
        src, dst = entry(kind, peer, h)
        return pltpu.make_async_remote_copy(
            src_ref=src, dst_ref=dst, send_sem=in_s.at[kind, r - 1], recv_sem=in_r.at[kind, r - 1],
            device_id={"head": peer}, device_id_type=MESH)

    def entry_own(kind):
        src, dst = entry(kind, h, h)
        return pltpu.make_async_copy(src, dst, loc_sem.at[kind])

    def entry_start(kind):
        entry_own(kind).start()
        for r in range(1, n):
            entry_copy(kind, r).start()

    for kind in range(1, first_wide):
        entry_start(kind)
    lse_rows = (lse_ref[...] * LOG2E).T
    for owner in range(n):
        st_ref[owner, 0:heads, :] = lse_rows[owner * heads : (owner + 1) * heads, :]
        for j in range(heads):
            hcol = pl.ds((owner * heads + j) * hd, hd)
            product = e_ref[:, hcol].astype(jnp.float32) * o_ref[:, hcol].astype(jnp.float32)
            st_ref[owner, heads + j : heads + j + 1, :] = jnp.sum(product.T, axis=0, keepdims=True)
    entry_start(first_wide)
    entry_start(0)
    for kind in range(first_wide + 1, kinds):
        entry_start(kind)

    def entry_wait(kind):
        entry_own(kind).wait()
        for r in range(1, n):
            entry_copy(kind, r).wait_recv()

    def hand(g, step, slot, to_slot, to):
        return pltpu.make_async_remote_copy(
            src_ref=kv.at[slot, g], dst_ref=kv.at[to_slot, g], send_sem=fw_s.at[g, step],
            recv_sem=fw_r.at[g, to_slot - 1], device_id={"seq": to}, device_id_type=MESH)

    def hand_steps(g):
        return (
            (has_up, hand(g, 0, 0, 2, s + 2)),
            (even, hand(g, 1, 0, 1, side)),
            (has_down & odd, hand(g, 2, 2, 1, side)),
            (has_down & even, hand(g, 2, 2, 3, side)),
            (has_down & even & has_up, hand(g, 3, 1, 3, s + 2)),
        )

    def hand_start(g, steps):
        for i in steps:
            cond, copy = hand_steps(g)[i]

            @pl.when(cond)
            def _():
                copy.start()

    def got(g, d):
        @pl.when(s >= d)
        def _():
            hand(g, 0, 0, d, side).wait_recv()

    def back(g, d, into, to):
        return pltpu.make_async_remote_copy(
            src_ref=part_s.at[g, d - 1], dst_ref=part_r.at[g, into], send_sem=pt_s.at[g, d - 1],
            recv_sem=pt_r.at[g, into], device_id={"seq": to}, device_id_type=MESH)

    def join(g, into):
        back(g, 1, into, side).wait_recv()
        acck[...] += part_r[g, into, 0].astype(jnp.float32)
        accv[...] += part_r[g, into, 1].astype(jnp.float32)

    def put(g, d):
        part_s[g, d - 1, 0] = acck[...].astype(jnp.bfloat16)
        part_s[g, d - 1, 1] = accv[...].astype(jnp.bfloat16)

    def pass_back(g, d):
        if d == 3:
            put(g, 3)

            @pl.when(even)
            def _():
                back(g, 3, 0, s - 2).start()

            @pl.when(odd)
            def _():
                back(g, 3, 1, side).start()
        elif d == 1:
            @pl.when(has_down & even & has_up)
            def _():
                join(g, 0)

            put(g, 1)

            @pl.when(even)
            def _():
                back(g, 1, 1, side).start()

            @pl.when(odd)
            def _():
                back(g, 1, 3, side).start()
        else:
            join(g, 1)
            put(g, 2)
            back(g, 2, 2, s - 2).start()

    def leave(which, g, owner):
        src, dst, size, full = ((dqs, dq_out, gw, cols), (dks, dk_out, hd, kcols), (dvs, dv_out, hd, kcols))[which]
        to_cols = pl.ds(pl.multiple_of(h * full + g * size, hd), size)
        return src.at[at(owner, rows), pl.ds(g * size, size)], dst.at[:, to_cols]

    def leave_copy(which, g, r):
        peer = lax.rem(h + r, n)
        src, dst = leave(which, g, peer)
        return pltpu.make_async_remote_copy(
            src_ref=src, dst_ref=dst, send_sem=out_s.at[which, g, r - 1], recv_sem=out_r.at[which, g, r - 1],
            device_id={"head": peer}, device_id_type=MESH)

    def leave_own(which, g):
        src, dst = leave(which, g, h)
        return pltpu.make_async_copy(src, dst, loc_sem.at[kinds + which * groups + g])

    def leave_start(which, g):
        for r in range(1, n):
            leave_copy(which, g, r).start()
        leave_own(which, g).start()

    for g in range(groups):
        entry_wait(1 + 2 * g)
        entry_wait(2 + 2 * g)
        hand_start(g, (0, 1))
    entry_wait(0)

    def relay_two(g):
        got(g, 2)
        hand_start(g, (2, 3))

    def relay_one(g):
        got(g, 1)
        hand_start(g, (4,))

    row_at = lax.broadcasted_iota(jnp.int32, (TILE, TILE), 0)
    col_at = lax.broadcasted_iota(jnp.int32, (TILE, TILE), 1)

    def tile(g, d, hf, qt):
        k_rows, q_rows = at(hf, TILE), at(qt, TILE)
        key, val = kv[d, g, 0, k_rows, :], kv[d, g, 1, k_rows, :]
        key_t = key.T
        first = start_ref[0:1, q_rows] - (hf * TILE - d * block)
        allowed = row_at >= first
        if d == 0:
            allowed &= row_at + (hf - qt) * TILE <= col_at
        add_k = add_v = None
        for m in range(width):
            hcol = pl.ds((g * width + m) * hd, hd)
            query, grad = qb[q_rows, hcol], eb[q_rows, hcol]
            lse = stb[g * width + m : g * width + m + 1, q_rows]
            delta = stb[heads + g * width + m : heads + g * width + m + 1, q_rows]
            scores = dot_nt(key, query)
            probs = jnp.exp2(jnp.where(allowed, scores * (scale * LOG2E) - lse, -jnp.inf))
            dprobs = dot_nt(val, grad)
            dscores = (probs * (dprobs - delta)).astype(jnp.bfloat16)
            one_v = dot(probs.astype(jnp.bfloat16), grad)
            one_k = dot(dscores, query)
            add_v = one_v if m == 0 else add_v + one_v
            add_k = one_k if m == 0 else add_k + one_k
            dqt[m, :, q_rows] += dot(key_t, dscores)
        acck[k_rows, :] += add_k
        accv[k_rows, :] += add_v

    def compute(g, d):
        acck[...] = jnp.zeros_like(acck)
        accv[...] = jnp.zeros_like(accv)

        for hf in range(halves):
            low = hf if d == 0 else 0
            high = hf + 1 if d == REACH else halves
            for qt in range(low, high):
                tile(g, d, hf, qt)

    def finish(g):
        for cond, into in ((even, 3), (has_up, 2)):
            @pl.when(cond)
            def _():
                back(g, 1, into, side).wait_recv()
                ownk[g] += part_r[g, into, 0].astype(jnp.float32)
                ownv[g] += part_r[g, into, 1].astype(jnp.float32)

        dks[:, g * hd : (g + 1) * hd] = (ownk[g] * scale).astype(jnp.bfloat16)
        dvs[:, g * hd : (g + 1) * hd] = ownv[g].astype(jnp.bfloat16)
        leave_start(1, g)
        leave_start(2, g)

    relay_two(0)
    for g in range(groups):
        if g == 0:
            relay_two(1)
            relay_one(0)
        entry_wait(first_wide + 2 * g)
        entry_wait(first_wide + 1 + 2 * g)
        dqt[...] = jnp.zeros_like(dqt)
        for step, d in enumerate((0, 3, 1, 2) if g == 0 else (3, 1, 2, 0)):
            if d == 0:
                compute(g, 0)
                ownk[g] = acck[...]
                ownv[g] = accv[...]
                if g == 0:
                    relay_one(1)
            else:
                if d == 3:
                    got(g, 3)

                @pl.when(s >= d)
                def _():
                    compute(g, d)
                    pass_back(g, d)
            if g > 0 and step == 1:
                finish(g - 1)
        for m in range(width):
            here = (g * width + m) * hd
            dqs[:, here : here + hd] = (dqt[m] * scale).T.astype(jnp.bfloat16)
        leave_start(0, g)
    finish(groups - 1)

    for which in range(3):
        for g in range(groups):
            leave_own(which, g).wait()
            for r in range(1, n):
                leave_copy(which, g, r).wait()
    for kind in range(kinds):
        for r in range(1, n):
            entry_copy(kind, r).wait_send()
    for g in range(groups):
        for cond, copy in hand_steps(g):
            @pl.when(cond)
            def _():
                copy.wait_send()

        for d in range(1, REACH + 1):
            @pl.when(s >= d)
            def _():
                back(g, d, 0, side).wait_send()


def shards(query, key, value, out, output_gradient, log_sum_exp, segment_ids):
    n, seqs = lax.axis_size("head"), lax.axis_size("seq")
    hd = HEAD_SIZE
    rows = query.shape[0]
    block = rows * n
    cols, kcols = query.shape[1] // n, key.shape[1] // n
    groups, width = kcols // hd, cols // kcols
    heads = groups * width
    base = lax.axis_index("seq") * block
    mine = lax.dynamic_slice_in_dim(segment_ids, base, block, 0)
    start = jnp.sum((segment_ids[:, None] < mine[None, :]).astype(jnp.int32), axis=0)[None, :] - base
    bf16, f32 = jnp.bfloat16, jnp.float32
    kinds = 1 + 4 * groups
    vmem = pl.BlockSpec(memory_space=pltpu.VMEM)
    dma = pltpu.SemaphoreType.DMA
    return pl.pallas_call(
        functools.partial(kernel, n, seqs, groups, width),
        out_shape=[
            jax.ShapeDtypeStruct(query.shape, bf16),
            jax.ShapeDtypeStruct(key.shape, bf16),
            jax.ShapeDtypeStruct(value.shape, bf16),
        ],
        in_specs=[vmem] * 7,
        out_specs=[vmem] * 3,
        scratch_shapes=[
            pltpu.VMEM((n, 2 * heads, rows), f32),
            pltpu.VMEM((block, cols), bf16),
            pltpu.VMEM((block, cols), bf16),
            pltpu.VMEM((2 * heads, block), f32),
            pltpu.VMEM((REACH + 1, groups, 2, block, hd), bf16),
            pltpu.VMEM((width, hd, block), f32),
            pltpu.VMEM((block, hd), f32),
            pltpu.VMEM((block, hd), f32),
            pltpu.VMEM((groups, block, hd), f32),
            pltpu.VMEM((groups, block, hd), f32),
            pltpu.VMEM((groups, REACH, 2, block, hd), bf16),
            pltpu.VMEM((groups, REACH + 1, 2, block, hd), bf16),
            pltpu.VMEM((block, cols), bf16),
            pltpu.VMEM((block, kcols), bf16),
            pltpu.VMEM((block, kcols), bf16),
            dma((kinds + 3 * groups,)),
            dma((kinds, n - 1)),
            dma((kinds, n - 1)),
            dma((groups, REACH + 1)),
            dma((groups, REACH)),
            dma((groups, REACH)),
            dma((groups, REACH + 1)),
            dma((3, groups, n - 1)),
            dma((3, groups, n - 1)),
        ],
        compiler_params=pltpu.CompilerParams(collective_id=0, has_side_effects=True),
    )(query, output_gradient, key, value, out, log_sum_exp, start)


def solution(mesh):
    placed = (P(("seq", "head"), None),) * 6 + (P(),)
    return jax.shard_map(
        lambda *a: tuple(shards(*a)),
        mesh=mesh,
        in_specs=placed,
        out_specs=(P(("seq", "head"), None),) * 3,
        check_vma=False,
    )
```
